32 devices in a mesh: expert: 8 (over z, x), mp: 4 (over y, core).
Axes of the slice: x: 2, y: 2, z: 4, core: 2. Of those that a mesh axis runs over, the one named last changes fastest.
Arguments:
- tokens: bfloat16 [192, 6144], P('expert', 'mp'), may hold values from -6 to 6
- mix_weights: float32 [192, 2], P('expert'), may hold values from 0.2 to 1
- routes: int32 [192, 2], P('expert'), may hold values from 0 to 7, as said below
- w_gate: bfloat16 [8, 6144, 8192], P('expert', None, 'mp'), may hold values from -0.078125 to 0.078125
- w_up: bfloat16 [8, 6144, 8192], P('expert', None, 'mp'), may hold values from -0.078125 to 0.078125
- w_down: bfloat16 [8, 8192, 6144], P('expert', 'mp'), may hold values from -0.0625 to 0.0625
Outputs:
- mixed_out: bfloat16 [192, 6144], P('expert', 'mp')
The draws below stay inside these ranges and needn't reach their ends.
Inputs may be any that keep to these rules, and one draw needn't show every extreme that they name: `routes`: each row names 2 different experts, and every expert is named by some row. Among the 24 rows of one index of the expert axis no expert is named more than 12 times, and on some indices one is named exactly 12 times.
All inputs are finite; a program needn't handle non-finite values.
Results may differ from the reference program's by a relative error of at most 0.011.
Values may be sent and summed in bfloat16 or wider, within the bound.
A program may use at most 128 MiB of HBM per device.

```python
import jax
import jax.numpy as jnp

D = 6144
FF = 8192
EXPERTS = 8
TOP = 2
TOK_DEV = 24
MOST = 12
GROUP = 1
FF_SLICE = 8192
TOKENS = 192
CAP = 60


def block_routes(block_key, busiest):
    order_key, rows_key, shift_key = jax.random.split(block_key, 3)
    others_order = jax.random.permutation(order_key, EXPERTS - 1).astype(jnp.int32)
    others = ((busiest + 1 + others_order) % EXPERTS).astype(jnp.int32)
    row_order = jax.random.permutation(rows_key, TOK_DEV).astype(jnp.int32)
    shift = jax.random.randint(shift_key, (), 0, EXPERTS - 2).astype(jnp.int32)
    first = jnp.where(row_order < MOST, busiest, others[0]).astype(jnp.int32)
    second_idx = (1 + (row_order + shift) % (EXPERTS - 2)).astype(jnp.int32)
    second = jnp.take(others, second_idx).astype(jnp.int32)
    return jnp.stack([first, second], axis=1).astype(jnp.int32)


def draw_routes(key, part):
    base = jax.random.fold_in(key, 4711)
    busiest = jax.random.randint(jax.random.fold_in(base, 99), (), 0, EXPERTS).astype(jnp.int32)
    block_count = TOKENS // TOK_DEV
    keys = jax.random.split(base, block_count)
    grids = jax.vmap(block_routes, in_axes=(0, None))(keys, busiest)
    return grids.reshape(TOKENS, TOP).astype(jnp.int32)


def level_of(stream_key, dims, cuts, least, largest):
    factor_of = 1.0
    for axis_at, shards_of in cuts:
        heights = jax.random.uniform(jax.random.fold_in(jax.random.fold_in(stream_key, 6), axis_at), (shards_of,), jnp.float32, least / len(cuts), largest / len(cuts))
        factor_of = factor_of * jnp.repeat(jnp.exp(heights), dims[axis_at] // shards_of).reshape((-1,) + (1,) * (len(dims) - 1 - axis_at))
    return factor_of


def bell_draw(stream_key, extent, deviation, bound, shards=(), kind=jnp.bfloat16):
    result = deviation * jax.random.normal(stream_key, extent, jnp.float32)
    if shards:
        result = result * level_of(stream_key, extent, shards, -0.22, 0.18)
    return jnp.clip(result, -bound, bound).astype(kind)


def setup_inputs(seed: int = 0) -> dict:
    streams_of = jax.random.split(jax.random.key(seed), 7)
    return {
        "tokens": bell_draw(streams_of[0], (TOKENS, D), 1.0, 6.0, ((0, 8), (1, 4))),
        "mix_weights": jnp.clip(0.2 + 0.8 * jax.random.uniform(streams_of[1], (TOKENS, TOP), jnp.float32) ** level_of(streams_of[1], (TOKENS, TOP), ((0, 8),), -0.2, 0.2), 0.2, 1.0),
        "routes": draw_routes(jax.random.fold_in(streams_of[6], 71), 0),
        "w_gate": bell_draw(streams_of[3], (EXPERTS * GROUP, D, FF_SLICE), D ** -0.5, 0.078125, ((0, 8), (2, 4))),
        "w_up": bell_draw(streams_of[4], (EXPERTS * GROUP, D, FF_SLICE), D ** -0.5, 0.078125, ((0, 8), (2, 4))),
        "w_down": bell_draw(streams_of[5], (EXPERTS * GROUP, FF_SLICE, D), FF ** -0.5, 0.0625, ((0, 8), (1, 4))),
    }


def assignment_slots(routes):
    flat_ids = routes.reshape(-1)
    labels = jnp.arange(EXPERTS, dtype=jnp.int32)
    marked = (flat_ids[:, None] == labels[None, :]).astype(jnp.int32)
    earlier = jnp.cumsum(marked, axis=0) - marked
    return flat_ids, jnp.sum(earlier * marked, axis=1).astype(jnp.int32)


def reference(tokens, mix_weights, routes, w_gate, w_up, w_down):
    flat_ids, slot_ids = assignment_slots(routes)
    token_ids = (jnp.arange(TOKENS * TOP, dtype=jnp.int32) // TOP).astype(jnp.int32)
    slot_grid = slot_ids.reshape(TOKENS, TOP)
    mixed_out = jnp.zeros((TOKENS, D), jnp.float32)
    for expert in range(EXPERTS):
        chosen = (flat_ids == expert) & (slot_ids < CAP)
        target = jnp.where(chosen, slot_ids, CAP).astype(jnp.int32)
        holder = jnp.zeros((CAP + 1,), jnp.int32).at[target].set(token_ids)[:CAP]
        filled = jnp.zeros((CAP + 1,), jnp.int32).at[target].set(1)[:CAP]
        slot_rows = jnp.where(filled[:, None] > 0, tokens[holder], jnp.zeros((), tokens.dtype))
        expert_out = jnp.zeros((CAP, D), jnp.float32)
        for member in range(GROUP):
            weight_row = expert * GROUP + member
            gate_act = jnp.dot(slot_rows, w_gate[weight_row], preferred_element_type=jnp.float32)
            up_act = jnp.dot(slot_rows, w_up[weight_row], preferred_element_type=jnp.float32)
            hidden = (jax.nn.silu(gate_act) * up_act).astype(jnp.bfloat16)
            part_sum = jnp.dot(hidden, w_down[weight_row], preferred_element_type=jnp.float32).astype(jnp.bfloat16)
            expert_out = expert_out + part_sum.astype(jnp.float32)
        for column in range(TOP):
            is_taken = (routes[:, column] == expert) & (slot_grid[:, column] < CAP)
            weight = jnp.where(is_taken, mix_weights[:, column], jnp.zeros((), jnp.float32))
            picked = jnp.take(expert_out, jnp.minimum(slot_grid[:, column], CAP - 1).astype(jnp.int32), axis=0)
            mixed_out = mixed_out + weight[:, None] * picked
    return mixed_out.astype(jnp.bfloat16)
```

```python
import functools

import jax
import jax.numpy as jnp
from jax import lax
from jax.experimental import pallas as pl
from jax.experimental.pallas import tpu as pltpu
from jax.sharding import PartitionSpec as P

EXPERTS = 8
TOP = 2
BLOCK = 16
LANES = 128
COLS = 256
MESH = pl.DeviceIdType.MESH


def fused(
    senders, capacity,
    tokens, mix, routes, w_gate, w_up, w_down, out,
    wbuf, packed, arrived, x, hidden, cnt_send, cnt_all, pick_w, compact,
    own, red_send, red_recv, ret_send, ret_recv,
    w_sem, d_sem, cs_sem, cr_sem, as_sem, ar_sem, ys_sem, yr_sem, ss_sem, sr_sem,
    rs_sem, rr_sem, ts_sem, tr_sem,
):
    me = lax.axis_index("expert")
    m = lax.axis_index("mp")
    sibling = m + 1 - 2 * lax.rem(m, 2)
    across = lax.rem(m + 2, 4)
    across_sibling = lax.rem(sibling + 2, 4)
    tok_rows = tokens.shape[0]
    depth, units = w_gate.shape[1], w_gate.shape[2] // COLS
    ff = w_down.shape[1]
    fit = depth // ff
    pieces = depth // COLS
    rounds = pieces // 4
    width = tokens.shape[1]
    slots = x.shape[0]

    def peer(d):
        return lax.rem(me + d, senders)

    def from_peer(d):
        return lax.rem(me + senders - d, senders)

    def remote(src, dst, send, recv, to_expert, to_mp):
        return pltpu.make_async_remote_copy(
            src_ref=src, dst_ref=dst, send_sem=send, recv_sem=recv,
            device_id=(to_expert, to_mp), device_id_type=MESH,
        )

    def gate_copy(n):
        return pltpu.make_async_copy(
            w_gate.at[0, :, pl.ds(pl.multiple_of(n * COLS, COLS), COLS)], wbuf.at[2 * n], w_sem.at[2 * n]
        )

    def up_copy(n):
        return pltpu.make_async_copy(
            w_up.at[0, :, pl.ds(pl.multiple_of(n * COLS, COLS), COLS)], wbuf.at[2 * n + 1], w_sem.at[2 * n + 1]
        )

    def piece_view(p):
        return wbuf.at[p // fit, pl.ds(pl.multiple_of(lax.rem(p, fit) * ff, ff), ff), :]

    def piece_copy(p):
        c, j = p // 4, lax.rem(p, 4)
        owner = lax.rem(m + 1 + j, 4)
        start = pl.multiple_of(owner * width + c * COLS, COLS)
        return pltpu.make_async_copy(
            w_down.at[0, :, pl.ds(start, COLS)], piece_view(p), d_sem.at[p]
        )

    def prefetch(n, carry):
        gate_copy(n).start()
        up_copy(n).start()
        return carry

    barrier = pltpu.get_barrier_semaphore()
    for d in range(1, senders):
        pl.semaphore_signal(barrier, inc=1, device_id=(peer(d), m), device_id_type=MESH)
    for d in range(1, 4):
        pl.semaphore_signal(
            barrier, inc=1, device_id=(me, lax.rem(m + d, 4)), device_id_type=MESH
        )
    lax.fori_loop(0, units, prefetch, 0)

    lane = lax.broadcasted_iota(jnp.int32, (tok_rows, LANES), 1)
    lane_expert, lane_rank = lane // BLOCK, lax.rem(lane, BLOCK)
    ids = routes[...]
    first = jnp.where(ids[:, 0:1] == lane_expert, 1.0, 0.0)
    second = jnp.where(ids[:, 1:2] == lane_expert, 1.0, 0.0)
    marked = first + second
    row_at = lax.broadcasted_iota(jnp.int32, (tok_rows, tok_rows), 0)
    col_at = lax.broadcasted_iota(jnp.int32, (tok_rows, tok_rows), 1)
    below = jnp.where(col_at < row_at, 1.0, 0.0).astype(jnp.bfloat16)
    earlier = jnp.dot(below, marked.astype(jnp.bfloat16), preferred_element_type=jnp.float32)
    pick = marked * jnp.where(earlier == lane_rank.astype(jnp.float32), 1.0, 0.0)
    cnt_send[...] = jnp.broadcast_to(jnp.sum(marked, axis=0, keepdims=True), cnt_send.shape)
    blocks = lax.dot_general(
        pick.astype(jnp.bfloat16), tokens[...], (((0,), (0,)), ((), ())),
        preferred_element_type=jnp.float32,
    ).astype(jnp.bfloat16).reshape(packed.shape)
    packed[...] = blocks
    arrived[m, me] = packed[me]
    cnt_all[me] = cnt_send[...]

    pl.semaphore_wait(barrier, senders - 1 + 3)

    def block_copy(d):
        return remote(packed.at[peer(d)], arrived.at[m, me], as_sem.at[d - 1], ar_sem.at[d - 1], peer(d), m)

    def count_copy(d):
        return remote(cnt_send, cnt_all.at[me], cs_sem.at[d - 1], cr_sem.at[d - 1], peer(d), m)

    def across_copy(d):
        block = arrived.at[m, from_peer(d)]
        return remote(block, block, ys_sem.at[d], yr_sem.at[d], me, across)

    def sibling_copy(d, which, at):
        block = arrived.at[which, from_peer(d)]
        return remote(block, block, ss_sem.at[at, d], sr_sem.at[at, d], me, sibling)

    for d in range(1, senders):
        block_copy(d).start()
    for d in range(1, senders):
        count_copy(d).start()
    for d in range(senders):
        if d:
            block_copy(d).wait_recv()
        across_copy(d).start()
        sibling_copy(d, m, 0).start()
    for d in range(senders):
        across_copy(d).wait_recv()
        sibling_copy(d, across, 1).start()
    for d in range(1, senders):
        count_copy(d).wait_recv()

    counts = cnt_all[:, 0, :]
    expert_lane = lax.broadcasted_iota(jnp.int32, (senders, LANES), 1)
    sender_row = lax.broadcasted_iota(jnp.int32, (senders, LANES), 0)
    mine = jnp.sum(jnp.where(expert_lane == me * BLOCK, counts, 0.0), axis=1, keepdims=True)
    block_of = expert_lane // BLOCK
    lane_cnt = jnp.sum(jnp.where(block_of == sender_row, mine, 0.0), axis=0, keepdims=True)
    lane_off = jnp.sum(jnp.where(sender_row < block_of, mine, 0.0), axis=0, keepdims=True)
    rank_f = lax.rem(lax.broadcasted_iota(jnp.int32, (slots, LANES), 1), BLOCK).astype(jnp.float32)
    slot_f = lax.broadcasted_iota(jnp.int32, (slots, LANES), 0).astype(jnp.float32)
    hit = jnp.where(rank_f < lane_cnt, 1.0, 0.0) * jnp.where(rank_f + lane_off == slot_f, 1.0, 0.0)
    hit = hit * jnp.where(slot_f < capacity, 1.0, 0.0)
    compact[...] = hit.astype(jnp.bfloat16)

    offset = jnp.sum(jnp.where(sender_row < me, counts, 0.0), axis=0, keepdims=True)
    weights = mix[...]
    weighted = pick * (first * weights[:, 0:1] + second * weights[:, 1:2])
    weighted = weighted * jnp.where(offset + earlier < capacity, 1.0, 0.0)
    high = weighted.astype(jnp.bfloat16)
    pick_w[0] = high
    pick_w[1] = (weighted - high.astype(jnp.float32)).astype(jnp.bfloat16)

    def gather(which):
        rows = arrived[which].reshape(senders * BLOCK, width)
        got = jnp.dot(compact[...], rows, preferred_element_type=jnp.float32)
        x[:, pl.ds(pl.multiple_of(which * width, width), width)] = got.astype(jnp.bfloat16)

    gather(m)
    gather(across)
    for d in range(senders):
        sibling_copy(d, m, 0).wait_recv()
    gather(sibling)
    for d in range(senders):
        sibling_copy(d, across, 1).wait_recv()
    gather(across_sibling)

    per_step = 2 * fit

    def middle(n, carry):
        gate_copy(n).wait()
        gate = jnp.dot(x[...], wbuf[2 * n], preferred_element_type=jnp.float32)
        up_copy(n).wait()
        up = jnp.dot(x[...], wbuf[2 * n + 1], preferred_element_type=jnp.float32)
        act = gate / (1.0 + jnp.exp(-gate)) * up
        hidden[:, pl.ds(pl.multiple_of(n * COLS, COLS), COLS)] = act.astype(jnp.bfloat16)

        @pl.when(n < pieces // per_step)
        def _():
            for i in range(per_step):
                piece_copy(n * per_step + i).start()

        return carry

    lax.fori_loop(0, units, middle, 0)

    def reduce_copy(c, j):
        owner = lax.rem(m + 1 + j, 4)
        return remote(red_send.at[c, j], red_recv.at[c, j], rs_sem.at[c, j], rr_sem.at[c, j], me, owner)

    def return_copy(c, d):
        return remote(ret_send.at[c, peer(d)], ret_recv.at[c, me], ts_sem.at[c, d - 1], tr_sem.at[c, d - 1], peer(d), m)

    def send_back(c):
        total = own[c]
        for j in range(3):
            reduce_copy(c, j).wait_recv()
            total = total + red_recv[c, j].astype(jnp.float32)
        spread = lax.dot_general(
            compact[...], total.astype(jnp.bfloat16), (((0,), (0,)), ((), ())),
            preferred_element_type=jnp.float32,
        ).astype(jnp.bfloat16)
        ret_send[c] = spread.reshape(senders, BLOCK, COLS)
        ret_recv[c, me] = ret_send[c, me]
        for d in range(1, senders):
            return_copy(c, d).start()

    lag = 2

    def down(c, carry):
        for j in range(4):
            p = c * 4 + j
            piece_copy(p).wait()
            rows = wbuf[p // fit, pl.ds(pl.multiple_of(lax.rem(p, fit) * ff, ff), ff), :]
            part = jnp.dot(hidden[...], rows, preferred_element_type=jnp.float32)
            if j < 3:
                red_send[c, j] = part.astype(jnp.bfloat16)
                reduce_copy(c, j).start()
            else:
                own[c] = part

        @pl.when(c >= lag)
        def _():
            send_back(c - lag)

        return carry

    lax.fori_loop(0, rounds, down, 0)

    def last(c, carry):
        send_back(c)
        return carry

    lax.fori_loop(rounds - lag, rounds, last, 0)

    def combine(c, carry):
        for d in range(1, senders):
            return_copy(c, d).wait_recv()
        rows = ret_recv[c].reshape(LANES, COLS)
        mixed = jnp.dot(pick_w[0], rows, preferred_element_type=jnp.float32)
        mixed = mixed + jnp.dot(pick_w[1], rows, preferred_element_type=jnp.float32)
        out[:, pl.ds(pl.multiple_of(c * COLS, COLS), COLS)] = mixed.astype(jnp.bfloat16)
        return carry

    lax.fori_loop(0, rounds, combine, 0)

    for d in range(1, senders):
        block_copy(d).wait_send()
        count_copy(d).wait_send()
    for d in range(senders):
        across_copy(d).wait_send()
        sibling_copy(d, m, 0).wait_send()
        sibling_copy(d, across, 1).wait_send()

    def drain(c, carry):
        for j in range(3):
            reduce_copy(c, j).wait_send()
        for d in range(1, senders):
            return_copy(c, d).wait_send()
        return carry

    lax.fori_loop(0, rounds, drain, 0)


def local_fused(tokens, mix_weights, routes, w_gate, w_up, w_down):
    tok_rows, width = tokens.shape
    senders = lax.axis_size("expert")
    capacity = 5 * tok_rows * senders * TOP // (4 * EXPERTS)
    slots = -(-capacity // BLOCK) * BLOCK
    depth, ff = w_gate.shape[1], w_gate.shape[2]
    units = ff // COLS
    pieces = depth // COLS
    rounds = pieces // 4
    bf16, f32 = jnp.bfloat16, jnp.float32
    dma = pltpu.SemaphoreType.DMA
    vmem = pl.BlockSpec(memory_space=pltpu.VMEM)
    hbm = pl.BlockSpec(memory_space=pl.ANY)
    return pl.pallas_call(
        functools.partial(fused, senders, capacity),
        out_shape=jax.ShapeDtypeStruct((tok_rows, width), bf16),
        in_specs=[vmem, vmem, vmem, hbm, hbm, hbm],
        out_specs=vmem,
        scratch_shapes=[
            pltpu.VMEM((2 * units, depth, COLS), bf16),
            pltpu.VMEM((senders, BLOCK, width), bf16),
            pltpu.VMEM((4, senders, BLOCK, width), bf16),
            pltpu.VMEM((slots, depth), bf16),
            pltpu.VMEM((slots, ff), bf16),
            pltpu.VMEM((8, LANES), f32),
            pltpu.VMEM((senders, 8, LANES), f32),
            pltpu.VMEM((2, tok_rows, LANES), bf16),
            pltpu.VMEM((slots, LANES), bf16),
            pltpu.VMEM((rounds, slots, COLS), f32),
            pltpu.VMEM((rounds, 3, slots, COLS), bf16),
            pltpu.VMEM((rounds, 3, slots, COLS), bf16),
            pltpu.VMEM((rounds, senders, BLOCK, COLS), bf16),
            pltpu.VMEM((rounds, senders, BLOCK, COLS), bf16),
            dma((2 * units,)),
            dma((pieces,)),
            dma((senders - 1,)),
            dma((senders - 1,)),
            dma((senders - 1,)),
            dma((senders - 1,)),
            dma((senders,)),
            dma((senders,)),
            dma((2, senders)),
            dma((2, senders)),
            dma((rounds, 3)),
            dma((rounds, 3)),
            dma((rounds, senders - 1)),
            dma((rounds, senders - 1)),
        ],
        compiler_params=pltpu.CompilerParams(
            collective_id=0, has_side_effects=True, vmem_limit_bytes=67_043_328
        ),
    )(tokens, mix_weights, routes, w_gate, w_up, w_down)


def fits(tokens, w_gate):
    senders, ways = lax.axis_size("expert"), lax.axis_size("mp")
    tok_rows, width = tokens.shape
    depth, ff = w_gate.shape[1], w_gate.shape[2]
    return (
        senders == EXPERTS
        and senders * BLOCK == LANES
        and ways == 4
        and tok_rows // 2 <= BLOCK
        and tok_rows % 8 == 0
        and width % COLS == 0
        and ff % COLS == 0
        and depth % ff == 0
        and (depth // COLS) % (2 * (depth // ff)) == 0
        and depth // COLS <= 2 * (ff // COLS) * (depth // ff)
        and width // COLS > 2
        and 4 * depth * ff <= 52 * 2**20
    )


def local_any(tokens, mix_weights, routes, w_gate, w_up, w_down):
    form = local_fused if fits(tokens, w_gate) else local
    return form(tokens, mix_weights, routes, w_gate, w_up, w_down)


def pack_rows(pick_tokens, features, repeats):
    packed = jnp.einsum(
        "tem,tc->emc", pick_tokens, features, preferred_element_type=jnp.float32
    ).astype(jnp.bfloat16)
    spread = jnp.broadcast_to(packed[:, None], (packed.shape[0], repeats) + packed.shape[1:])
    return spread.reshape((packed.shape[0] * repeats,) + packed.shape[1:])


def activate(gate_act, up_act):
    return (jax.nn.silu(gate_act) * up_act).astype(jnp.bfloat16)


def local(tokens, mix_weights, routes, w_gate, w_up, w_down):
    tok_rows = tokens.shape[0]
    senders = lax.axis_size("expert")
    group_size = senders // EXPERTS
    capacity = 5 * tok_rows * senders * TOP // (4 * EXPERTS)
    most_rows = tok_rows // 2
    labels = jnp.arange(EXPERTS, dtype=jnp.int32)
    flat_ids = routes.reshape(-1)
    marked = (flat_ids[:, None] == labels[None, :]).astype(jnp.int32)
    earlier = jnp.cumsum(marked, axis=0) - marked
    local_rank = jnp.sum(earlier * marked, axis=1)
    counts = jnp.sum(marked, axis=0)
    count_grid = lax.all_gather(counts[None, :], "expert", axis=0, tiled=True)
    my_index = lax.axis_index("expert")
    sender_ids = jnp.arange(senders, dtype=jnp.int32)
    lower_mask = (sender_ids[:, None] < my_index).astype(jnp.int32)
    offsets = jnp.sum(count_grid * lower_mask, axis=0)
    slot_ids = jnp.sum(marked * offsets[None, :], axis=1) + local_rank
    keep_mask = (slot_ids < capacity).astype(jnp.int32)
    rank_hit = (local_rank[:, None] == jnp.arange(most_rows, dtype=jnp.int32)[None, :]).astype(
        jnp.int32
    ) * keep_mask[:, None]
    assign_pick = marked[:, :, None] * rank_hit[:, None, :]
    pick_tokens = jnp.sum(assign_pick.reshape(tok_rows, TOP, EXPERTS, most_rows), axis=1).astype(
        jnp.bfloat16
    )
    weighted = assign_pick.astype(jnp.float32) * mix_weights.reshape(-1)[:, None, None]
    combine_w = jnp.sum(weighted.reshape(tok_rows, TOP, EXPERTS * most_rows), axis=1)
    gate_rows = w_gate[0]
    up_rows = w_up[0]
    down_rows = w_down[0]
    arrived = lax.all_to_all(
        pack_rows(pick_tokens, tokens, group_size),
        "expert",
        split_axis=0,
        concat_axis=0,
        tiled=True,
    )
    arrived_rows = arrived.reshape(senders * most_rows, arrived.shape[2])
    shard_piece = lax.all_gather(arrived_rows, "mp", axis=1, tiled=True)
    gate_act = jnp.dot(shard_piece, gate_rows, preferred_element_type=jnp.float32)
    up_act = jnp.dot(shard_piece, up_rows, preferred_element_type=jnp.float32)
    hidden = activate(gate_act, up_act)
    part_sum = jnp.dot(hidden, down_rows, preferred_element_type=jnp.float32)
    reduced = lax.psum_scatter(part_sum, "mp", scatter_dimension=1, tiled=True).astype(jnp.bfloat16)
    out_width = reduced.shape[1]
    returned = lax.all_to_all(
        reduced.reshape(senders, most_rows, out_width),
        "expert",
        split_axis=0,
        concat_axis=0,
        tiled=True,
    )
    summed = jnp.sum(
        returned.reshape(EXPERTS, group_size, most_rows, out_width).astype(jnp.float32), axis=1
    )
    result = jnp.dot(
        combine_w, summed.reshape(EXPERTS * most_rows, out_width), precision=lax.Precision.HIGHEST
    )
    return result.astype(jnp.bfloat16)


def solution(mesh):
    placed = (
        P("expert", "mp"),
        P("expert", None),
        P("expert", None),
        P("expert", None, "mp"),
        P("expert", None, "mp"),
        P("expert", "mp", None),
    )
    return jax.shard_map(
        local_any, mesh=mesh, in_specs=placed, out_specs=P("expert", "mp"), check_vma=False
    )
```
